32 devices in a mesh: blk: 8 (over y, x, core), row: 4 (over z).
Axes of the slice: x: 2, y: 2, z: 4, core: 2. Of those that a mesh axis runs over, the one named last changes fastest.
Arguments:
- rank_start: float32 [512, 128], P(('blk', 'row')), may hold values from 0.5 to 1.5
- tiles: bfloat16 [1024, 128, 128], P(('blk', 'row')), may hold values from 0 to 1
- tile_dest: int32 [1024], P(('blk', 'row')), may hold values from 0 to 63
- tile_src: int32 [1024], P(('blk', 'row')), may hold values from 0 to 127
- tile_fill: int32 [1024], P(('blk', 'row')), may hold values from 0 to 128
- out_degree: int32 [512, 128], P(('blk', 'row')), may hold values from 64 to 255
- dangling: int32 [512, 128], P(('blk', 'row')), may hold values 0 or 1
Outputs:
- rank: float32 [512, 128], P(('blk', 'row'))
- changes: float32 [2], replicated
The draws below stay inside these ranges and needn't reach their ends.
Inputs may be any that keep to these rules, and one draw needn't show every extreme that they name: `tile_fill`: 0 marks an empty slot.
All inputs are finite; a program needn't handle non-finite values. No bound on the sum of `dangling` on one device may be relied on, other than what follows from the above.
Results may differ from the reference program's by a relative error of at most 0.0003.
Values may be sent and summed in bfloat16 or wider, within the bound.
A program may use at most 64 MiB of HBM per device.

```python
import jax
import jax.numpy as jnp
from jax import lax

TILE = 128
SH = 16
K = 32
ITERS = 2
PAGE_TILES = 512
SLOTS = 1024
N_BLK = 8
N_ROW = 4


def with_ends(drawn, key, low, top_value):
    place = [jax.random.randint(jax.random.fold_in(key, axis), (), 0, length) for axis, length in enumerate(drawn.shape)]
    widest = drawn.shape.index(max(drawn.shape))
    beside = place[:widest] + [(place[widest] + 1) % drawn.shape[widest]] + place[widest + 1:]
    return drawn.at[tuple(place)].set(low).at[tuple(beside)].set(top_value)


def block_scale(rng, extent, shards, low, top_value):
    def one(position, blocks):
        heights = jax.random.uniform(jax.random.fold_in(jax.random.fold_in(rng, 6), position), (blocks,), jnp.float32, low / len(shards), top_value / len(shards))
        return jnp.repeat(jnp.exp(heights), extent[position] // blocks).reshape((-1,) + (1,) * (len(extent) - position - 1))

    loudness = one(*shards[0])
    for cut in shards[1:]:
        loudness = loudness * one(*cut)
    return loudness


def setup_inputs(seed: int = 0) -> dict:
    arg_keys = jax.random.split(jax.random.key(seed), 8)
    return {
        "rank_start": jnp.clip(0.5 + 1.0 * jax.random.uniform(arg_keys[0], (PAGE_TILES, TILE), jnp.float32) ** block_scale(arg_keys[0], (PAGE_TILES, TILE), ((0, 32),), -0.2, 0.2), 0.5, 1.5),
        "tiles": jnp.clip(1.0 * jax.random.uniform(arg_keys[1], (SLOTS, TILE, TILE), jnp.float32) ** block_scale(arg_keys[1], (SLOTS, TILE, TILE), ((0, 32),), -0.2, 0.2), 0.0, 1.0).astype(jnp.bfloat16),
        "tile_dest": with_ends(jax.random.randint(arg_keys[2], (SLOTS,), 0, N_ROW * SH), jax.random.fold_in(arg_keys[2], 1), 0, (N_ROW * SH) - 1).astype(jnp.int32),
        "tile_src": with_ends(jax.random.randint(arg_keys[3], (SLOTS,), 0, N_BLK * SH), jax.random.fold_in(arg_keys[3], 1), 0, (N_BLK * SH) - 1).astype(jnp.int32),
        "tile_fill": with_ends(jax.random.randint(arg_keys[4], (SLOTS,), 0, 129), jax.random.fold_in(arg_keys[4], 1), 0, 128).astype(jnp.int32),
        "out_degree": with_ends(jax.random.randint(arg_keys[5], (PAGE_TILES, TILE), 32 * K // SH, 128 * K // SH), jax.random.fold_in(arg_keys[5], 1), 32 * K // SH, (128 * K // SH) - 1).astype(jnp.int32),
        "dangling": with_ends((jax.random.randint(arg_keys[6], (PAGE_TILES, TILE), 0, 8) < 1).astype(jnp.int32), jax.random.fold_in(arg_keys[6], 1), 0, 1),
    }


damping = 0.85


def reference(rank_start, tiles, tile_dest, tile_src, tile_fill, out_degree, dangling):
    groups = N_BLK * N_ROW
    tile_sets = tiles.reshape(groups, K, TILE, TILE)
    dest_sets = tile_dest.reshape(groups, K)
    source_sets = tile_src.reshape(groups, K)
    fill_sets = tile_fill.reshape(groups, K)
    dangle = dangling.astype(jnp.float32)
    weight = (1.0 - dangle) / out_degree.astype(jnp.float32)
    page_total = groups * SH * TILE
    lane_index = jnp.arange(TILE, dtype=jnp.int32)
    rank = rank_start
    change_list = []
    for iteration in range(ITERS):
        lost_mass = jnp.sum(rank * dangle)
        scaled = (rank * weight).astype(jnp.bfloat16)

        def one_group(incoming, index):
            block_index = index // N_ROW
            row_index = index % N_ROW
            source_ids = source_sets[index]
            global_src = ((source_ids // SH) * (N_ROW * SH) + row_index * SH + source_ids % SH).astype(jnp.int32)
            sources = scaled[global_src]
            column_mask = lane_index[None, :] < fill_sets[index][:, None]
            sources = jnp.where(column_mask, sources, jnp.zeros_like(sources))
            products = jnp.einsum("kij,kj->ki", tile_sets[index].astype(jnp.float32), sources.astype(jnp.float32))
            global_dest = (block_index * (N_ROW * SH) + dest_sets[index]).astype(jnp.int32)
            return incoming.at[global_dest].add(products), None

        incoming, unused = lax.scan(one_group, jnp.zeros(rank.shape, jnp.float32), jnp.arange(groups, dtype=jnp.int32))
        updated = damping * incoming + (1.0 - damping) + damping * lost_mass / page_total
        change_list.append(jnp.sum(jnp.abs(updated - rank)))
        rank = updated
    return rank, jnp.stack(change_list)
```

```python
import functools

import jax
import jax.numpy as jnp
from jax import lax
from jax.experimental import pallas as pl
from jax.experimental.pallas import tpu as pltpu
from jax.sharding import PartitionSpec as P

ITERS = 2
UNROLL_LIMIT = 32

damping = 0.85


def each(count, body):
    if count <= UNROLL_LIMIT:
        for i in range(count):
            body(i)
    else:

        @pl.loop(0, count)
        def _(i):
            body(i)


def kernel(
    n_blk, n_row,
    rank_hbm, tiles_hbm, dest_hbm, src_hbm, fill_hbm, degree_hbm, dangling_hbm,
    rank_out, change_out,
    rank_v, tiles_v, degree_v, dangling_v, dest_s, src_s, fill_s,
    weight_v, dangle_v, spread_v, picked_v,
    pages, blk_stats, partial, shares, row_stats, in_sems, blk_sems, row_sems,
):
    b = lax.axis_index("blk")
    w = lax.axis_index("row")
    share, lanes = rank_v.shape
    slots = tiles_v.shape[0]
    page_total = n_blk * n_row * share * lanes

    def peer(axis, d):
        if axis == "blk":
            return {"blk": lax.rem(b + d, n_blk)}
        return {"row": lax.rem(w + d, n_row)}

    barrier = pltpu.get_barrier_semaphore()
    for axis, count in (("blk", n_blk), ("row", n_row)):
        each(count - 1, lambda i, axis=axis: pl.semaphore_signal(
            barrier, inc=1, device_id=peer(axis, i + 1),
            device_id_type=pl.DeviceIdType.MESH))

    loads = [
        pltpu.make_async_copy(source, target, in_sems.at[i])
        for i, (source, target) in enumerate((
            (rank_hbm, rank_v), (degree_hbm, degree_v), (dangling_hbm, dangling_v),
            (src_hbm, src_s), (dest_hbm, dest_s), (fill_hbm, fill_s), (tiles_hbm, tiles_v),
        ))
    ]
    for load in loads:
        load.start()
    for load in loads[:3]:
        load.wait()

    def send(axis, count, source, target, sems):
        def one(i):
            d = i + 1
            pltpu.make_async_remote_copy(
                src_ref=source(d), dst_ref=target.at[d],
                send_sem=sems.at[0], recv_sem=sems.at[1],
                device_id=peer(axis, d), device_id_type=pl.DeviceIdType.MESH,
            ).start()

        each(count - 1, one)

    def wait(count, target, sems, which):
        others = target.at[pl.ds(1, count - 1)]
        pltpu.make_async_copy(others, others, sems.at[which]).wait()

    sent = []

    def blk_send(source, target, sems):
        send("blk", n_blk, source, target, sems)
        sent.append((n_blk, target, sems))

    def row_send(source, target, sems):
        send("row", n_row, source, target, sems)
        sent.append((n_row, target, sems))

    def lane_sum(value):
        return jnp.sum(value, axis=0, keepdims=True)

    dangle = dangling_v[...].astype(jnp.float32)
    weight = (1.0 - dangle) / degree_v[...].astype(jnp.float32)
    weight_v[...] = weight
    dangle_v[...] = dangle
    rank = rank_v[...]
    pages[0, 0] = (rank * weight).astype(jnp.bfloat16)
    blk_stats[0, 0] = jnp.concatenate([lane_sum(rank * dangle), jnp.zeros((1, lanes), jnp.float32)], axis=0)
    pl.semaphore_wait(barrier, n_blk + n_row - 2)

    select = None
    for it in range(ITERS):
        blk_send(lambda d: pages.at[it, 0], pages.at[it], blk_sems.at[it, 0])
        blk_send(lambda d: blk_stats.at[it, 0], blk_stats.at[it], blk_sems.at[it, 1])

        if it == 0:
            for load in loads[3:6]:
                load.wait()
            slot_row = lax.broadcasted_iota(jnp.int32, (slots, n_blk * share), 0)
            slot_col = lax.broadcasted_iota(jnp.int32, (slots, n_blk * share), 1)
            source_row = jnp.zeros((slots, n_blk * share), jnp.int32)
            dest_row = lax.broadcasted_iota(jnp.int32, (n_row * share, lanes), 0)
            lane = lax.broadcasted_iota(jnp.int32, (n_row * share, lanes), 1)
            for k in range(slots):
                source = src_s[k]
                place = lax.rem(b - lax.div(source, share) + n_blk, n_blk) * share + lax.rem(source, share)
                source_row = jnp.where(slot_row == k, place, source_row)
                keep = (dest_row == dest_s[k]) & (lane < fill_s[k])
                spread_v[k] = jnp.where(keep, 1.0, 0.0)
            select = jnp.where(source_row == slot_col, 1.0, 0.0).astype(jnp.bfloat16)
            loads[6].wait()

        wait(n_blk, pages.at[it], blk_sems.at[it, 0], 1)
        picked_v[...] = jnp.dot(
            select, pages[it].reshape(n_blk * share, lanes), preferred_element_type=jnp.float32
        )
        total = jnp.zeros((n_row * share, lanes), jnp.float32)
        for k in range(slots):
            left = (spread_v[k] * picked_v[k:k + 1, :]).astype(jnp.bfloat16)
            total = total + lax.dot_general(
                left, tiles_v[k], (((1,), (1,)), ((), ())), preferred_element_type=jnp.float32
            )
        partial[it] = total.reshape(n_row, share, lanes)
        row_send(lambda d: partial.at[it, lax.rem(w + d, n_row)], shares.at[it], row_sems.at[it, 0])
        wait(n_blk, blk_stats.at[it], blk_sems.at[it, 1], 1)
        row_stats[it, 0] = jnp.sum(blk_stats[it], axis=0)
        row_send(lambda d: row_stats.at[it, 0], row_stats.at[it], row_sems.at[it, 1])
        own = partial[it, w]
        wait(n_row, row_stats.at[it], row_sems.at[it, 1], 1)
        stats = jnp.sum(jnp.sum(row_stats[it], axis=0), axis=1, keepdims=True)
        if it > 0:
            change_out[0:1, :] = jnp.broadcast_to(stats[1:2, :], (1, lanes))
        wait(n_row, shares.at[it], row_sems.at[it, 0], 1)
        incoming = own + jnp.sum(shares[it, 1:], axis=0)
        updated = damping * incoming + (1.0 - damping) + damping * stats[0:1, :] / page_total
        rank = rank_v[...]
        if it == 0:
            rank_v[...] = updated
            pages[it + 1, 0] = (updated * weight_v[...]).astype(jnp.bfloat16)
        else:
            rank_out[...] = updated
        blk_stats[it + 1, 0] = jnp.concatenate(
            [lane_sum(updated * dangle_v[...]), lane_sum(jnp.abs(updated - rank))], axis=0
        )

    blk_send(lambda d: blk_stats.at[ITERS, 0], blk_stats.at[ITERS], blk_sems.at[ITERS, 1])
    wait(n_blk, blk_stats.at[ITERS], blk_sems.at[ITERS, 1], 1)
    row_stats[ITERS, 0] = jnp.sum(blk_stats[ITERS], axis=0)
    row_send(lambda d: row_stats.at[ITERS, 0], row_stats.at[ITERS], row_sems.at[ITERS, 1])
    wait(n_row, row_stats.at[ITERS], row_sems.at[ITERS, 1], 1)
    stats = jnp.sum(jnp.sum(row_stats[ITERS], axis=0), axis=1, keepdims=True)
    change_out[1:2, :] = jnp.broadcast_to(stats[1:2, :], (1, lanes))
    for count, target, sems in sent:
        wait(count, target, sems, 0)


def solution(mesh):
    placed = (
        P(("blk", "row"), None),
        P(("blk", "row"), None, None),
        P(("blk", "row")),
        P(("blk", "row")),
        P(("blk", "row")),
        P(("blk", "row"), None),
        P(("blk", "row"), None),
    )
    n_blk, n_row = mesh.shape["blk"], mesh.shape["row"]

    def local(rank_start, tiles, tile_dest, tile_src, tile_fill, out_degree, dangling):
        share, lanes = rank_start.shape
        slots = tiles.shape[0]
        rank, changes = pl.pallas_call(
            functools.partial(kernel, n_blk, n_row),
            out_shape=(
                jax.ShapeDtypeStruct((share, lanes), jnp.float32),
                jax.ShapeDtypeStruct((2, lanes), jnp.float32),
            ),
            in_specs=[pl.BlockSpec(memory_space=pl.ANY)] * 7,
            out_specs=(pl.BlockSpec(memory_space=pltpu.VMEM),) * 2,
            scratch_shapes=[
                pltpu.VMEM((share, lanes), jnp.float32),
                pltpu.VMEM(tiles.shape, jnp.bfloat16),
                pltpu.VMEM((share, lanes), jnp.int32),
                pltpu.VMEM((share, lanes), jnp.int32),
                pltpu.SMEM((slots,), jnp.int32),
                pltpu.SMEM((slots,), jnp.int32),
                pltpu.SMEM((slots,), jnp.int32),
                pltpu.VMEM((share, lanes), jnp.float32),
                pltpu.VMEM((share, lanes), jnp.float32),
                pltpu.VMEM((slots, n_row * share, lanes), jnp.float32),
                pltpu.VMEM((slots, lanes), jnp.float32),
                pltpu.VMEM((ITERS, n_blk, share, lanes), jnp.bfloat16),
                pltpu.VMEM((ITERS + 1, n_blk, 2, lanes), jnp.float32),
                pltpu.VMEM((ITERS, n_row, share, lanes), jnp.float32),
                pltpu.VMEM((ITERS, n_row, share, lanes), jnp.float32),
                pltpu.VMEM((ITERS + 1, n_row, 2, lanes), jnp.float32),
                pltpu.SemaphoreType.DMA((7,)),
                pltpu.SemaphoreType.DMA((ITERS + 1, 2, 2)),
                pltpu.SemaphoreType.DMA((ITERS + 1, 2, 2)),
            ],
            compiler_params=pltpu.CompilerParams(collective_id=0, has_side_effects=True),
        )(rank_start, tiles, tile_dest, tile_src, tile_fill, out_degree, dangling)
        return rank, changes[:, 0]

    return jax.shard_map(
        local, mesh=mesh, in_specs=placed, out_specs=(P(("blk", "row"), None), P()), check_vma=False
    )
```

```python
import functools

import jax
import jax.numpy as jnp
from jax import lax
from jax.experimental import pallas as pl
from jax.experimental.pallas import tpu as pltpu
from jax.sharding import PartitionSpec as P

ITERS = 2
UNROLL_LIMIT = 32

damping = 0.85


def each(count, body):
    if count <= UNROLL_LIMIT:
        for i in range(count):
            body(i)
    else:

        @pl.loop(0, count)
        def _(i):
            body(i)


def finish(rank_ref, change_ref, rank_hbm, change_hbm, change_s, sems):
    write_rank = pltpu.make_async_copy(rank_ref, rank_hbm, sems.at[0])
    write_rank.start()
    for i in range(ITERS):
        change_s[i] = jnp.max(change_ref[i:i + 1, :])
    write_change = pltpu.make_async_copy(change_s, change_hbm, sems.at[1])
    write_change.start()
    write_rank.wait()
    write_change.wait()


def kernel(
    n_blk, n_row,
    rank_hbm, tiles_hbm, dest_hbm, src_hbm, fill_hbm, degree_hbm, dangling_hbm,
    rank_out, change_out,
    rank_v, tiles_v, degree_v, dangling_v, dest_s, src_s, fill_s,
    weight_v, dangle_v, spread_v, picked_v,
    pages, blk_stats, partial, shares, row_stats, last_stats, in_sems, blk_sems, row_sems, last_sems,
):
    b = lax.axis_index("blk")
    w = lax.axis_index("row")
    share, lanes = rank_v.shape
    slots = tiles_v.shape[0]
    page_total = n_blk * n_row * share * lanes

    def peer(axis, d):
        if axis == "blk":
            return {"blk": lax.rem(b + d, n_blk)}
        if axis == "row":
            return {"row": lax.rem(w + d, n_row)}
        return {"blk": lax.rem(b + d // n_row, n_blk), "row": lax.rem(w + d % n_row, n_row)}

    barrier = pltpu.get_barrier_semaphore()
    for axis, count in (("blk", n_blk), ("row", n_row)):
        each(count - 1, lambda i, axis=axis: pl.semaphore_signal(
            barrier, inc=1, device_id=peer(axis, i + 1),
            device_id_type=pl.DeviceIdType.MESH))

    loads = [
        pltpu.make_async_copy(source, target, in_sems.at[i])
        for i, (source, target) in enumerate((
            (rank_hbm, rank_v), (degree_hbm, degree_v), (dangling_hbm, dangling_v),
            (src_hbm, src_s), (dest_hbm, dest_s), (fill_hbm, fill_s), (tiles_hbm, tiles_v),
        ))
    ]
    for load in loads:
        load.start()
    for load in loads[:3]:
        load.wait()

    def send(axis, count, source, target, sems):
        def one(i):
            d = i + 1
            pltpu.make_async_remote_copy(
                src_ref=source(d), dst_ref=target.at[d],
                send_sem=sems.at[0], recv_sem=sems.at[1],
                device_id=peer(axis, d), device_id_type=pl.DeviceIdType.MESH,
            ).start()

        each(count - 1, one)

    def wait(count, target, sems, which):
        others = target.at[pl.ds(1, count - 1)]
        pltpu.make_async_copy(others, others, sems.at[which]).wait()

    sent = []

    def blk_send(source, target, sems):
        send("blk", n_blk, source, target, sems)
        sent.append((n_blk, target, sems))

    def row_send(source, target, sems):
        send("row", n_row, source, target, sems)
        sent.append((n_row, target, sems))

    def lane_sum(value):
        return jnp.sum(value, axis=0, keepdims=True)

    dangle = dangling_v[...].astype(jnp.float32)
    weight = (1.0 - dangle) / degree_v[...].astype(jnp.float32)
    weight_v[...] = weight
    dangle_v[...] = dangle
    rank = rank_v[...]
    pages[0, 0] = (rank * weight).astype(jnp.bfloat16)
    blk_stats[0, 0] = jnp.concatenate([lane_sum(rank * dangle), jnp.zeros((1, lanes), jnp.float32)], axis=0)
    pl.semaphore_wait(barrier, n_blk + n_row - 2)

    select = None
    for it in range(ITERS):
        blk_send(lambda d: pages.at[it, 0], pages.at[it], blk_sems.at[it, 0])
        blk_send(lambda d: blk_stats.at[it, 0], blk_stats.at[it], blk_sems.at[it, 1])

        if it == 0:
            for load in loads[3:6]:
                load.wait()
            slot_row = lax.broadcasted_iota(jnp.int32, (slots, n_blk * share), 0)
            slot_col = lax.broadcasted_iota(jnp.int32, (slots, n_blk * share), 1)
            source_row = jnp.zeros((slots, n_blk * share), jnp.int32)
            dest_row = lax.broadcasted_iota(jnp.int32, (n_row * share, lanes), 0)
            lane = lax.broadcasted_iota(jnp.int32, (n_row * share, lanes), 1)
            for k in range(slots):
                source = src_s[k]
                place = lax.rem(b - lax.div(source, share) + n_blk, n_blk) * share + lax.rem(source, share)
                source_row = jnp.where(slot_row == k, place, source_row)
                keep = (dest_row == dest_s[k]) & (lane < fill_s[k])
                spread_v[k] = jnp.where(keep, 1.0, 0.0)
            select = jnp.where(source_row == slot_col, 1.0, 0.0).astype(jnp.bfloat16)
            loads[6].wait()

        wait(n_blk, pages.at[it], blk_sems.at[it, 0], 1)
        picked_v[...] = jnp.dot(
            select, pages[it].reshape(n_blk * share, lanes), preferred_element_type=jnp.float32
        )
        wait(n_blk, blk_stats.at[it], blk_sems.at[it, 1], 1)
        row_stats[it, 0] = jnp.sum(blk_stats[it], axis=0)
        row_send(lambda d: row_stats.at[it, 0], row_stats.at[it], row_sems.at[it, 1])
        totals = [jnp.zeros((n_row * share, lanes), jnp.float32) for _ in range(2)]
        for k in range(0, slots, 2):
            left = jnp.concatenate([spread_v[k + i] * picked_v[k + i:k + i + 1, :] for i in range(2)], axis=1)
            right = jnp.concatenate([tiles_v[k + i] for i in range(2)], axis=1)
            half = k // 2 % 2
            totals[half] = totals[half] + lax.dot_general(
                left.astype(jnp.bfloat16), right, (((1,), (1,)), ((), ())), preferred_element_type=jnp.float32
            )
        partial[it] = (totals[0] + totals[1]).reshape(n_row, share, lanes)
        row_send(lambda d: partial.at[it, lax.rem(w + d, n_row)], shares.at[it], row_sems.at[it, 0])
        own = partial[it, w]
        wait(n_row, row_stats.at[it], row_sems.at[it, 1], 1)
        stats = jnp.sum(jnp.sum(row_stats[it], axis=0), axis=1, keepdims=True)
        if it > 0:
            change_out[0:1, :] = jnp.broadcast_to(stats[1:2, :], (1, lanes))
        base = (1.0 - damping) + damping * stats[0:1, :] / page_total
        wait(n_row, shares.at[it], row_sems.at[it, 0], 1)
        incoming = own + jnp.sum(shares[it, 1:], axis=0)
        updated = damping * incoming + base
        rank = rank_v[...]
        if it == 0:
            rank_v[...] = updated
            pages[it + 1, 0] = (updated * weight_v[...]).astype(jnp.bfloat16)
            blk_stats[it + 1, 0] = jnp.concatenate(
                [lane_sum(updated * dangle_v[...]), lane_sum(jnp.abs(updated - rank))], axis=0
            )
        else:
            last_stats[0] = lane_sum(jnp.abs(updated - rank))
            rank_out[...] = updated

    send("all", n_blk * n_row, lambda d: last_stats.at[0], last_stats, last_sems)
    sent.append((n_blk * n_row, last_stats, last_sems))
    wait(n_blk * n_row, last_stats, last_sems, 1)
    last = jnp.sum(jnp.sum(last_stats[...], axis=0), axis=1, keepdims=True)
    change_out[1:2, :] = jnp.broadcast_to(last, (1, lanes))
    for count, target, sems in sent:
        wait(count, target, sems, 0)


def solution(mesh):
    placed = (
        P(("blk", "row"), None),
        P(("blk", "row"), None, None),
        P(("blk", "row")),
        P(("blk", "row")),
        P(("blk", "row")),
        P(("blk", "row"), None),
        P(("blk", "row"), None),
    )
    n_blk, n_row = mesh.shape["blk"], mesh.shape["row"]

    def local(rank_start, tiles, tile_dest, tile_src, tile_fill, out_degree, dangling):
        share, lanes = rank_start.shape
        slots = tiles.shape[0]
        rank, changes = pl.pallas_call(
            functools.partial(kernel, n_blk, n_row),
            out_shape=(
                pltpu.VMEM((share, lanes), jnp.float32),
                pltpu.VMEM((ITERS, lanes), jnp.float32),
            ),
            in_specs=[pl.BlockSpec(memory_space=pl.ANY)] * 7,
            out_specs=(pl.BlockSpec(memory_space=pltpu.VMEM),) * 2,
            scratch_shapes=[
                pltpu.VMEM((share, lanes), jnp.float32),
                pltpu.VMEM(tiles.shape, jnp.bfloat16),
                pltpu.VMEM((share, lanes), jnp.int32),
                pltpu.VMEM((share, lanes), jnp.int32),
                pltpu.SMEM((slots,), jnp.int32),
                pltpu.SMEM((slots,), jnp.int32),
                pltpu.SMEM((slots,), jnp.int32),
                pltpu.VMEM((share, lanes), jnp.float32),
                pltpu.VMEM((share, lanes), jnp.float32),
                pltpu.VMEM((slots, n_row * share, lanes), jnp.float32),
                pltpu.VMEM((slots, lanes), jnp.float32),
                pltpu.VMEM((ITERS, n_blk, share, lanes), jnp.bfloat16),
                pltpu.VMEM((ITERS, n_blk, 2, lanes), jnp.float32),
                pltpu.VMEM((ITERS, n_row, share, lanes), jnp.float32),
                pltpu.VMEM((ITERS, n_row, share, lanes), jnp.float32),
                pltpu.VMEM((ITERS, n_row, 2, lanes), jnp.float32),
                pltpu.VMEM((n_blk * n_row, 1, lanes), jnp.float32),
                pltpu.SemaphoreType.DMA((7,)),
                pltpu.SemaphoreType.DMA((ITERS, 2, 2)),
                pltpu.SemaphoreType.DMA((ITERS, 2, 2)),
                pltpu.SemaphoreType.DMA((2,)),
            ],
            compiler_params=pltpu.CompilerParams(collective_id=0, has_side_effects=True),
        )(rank_start, tiles, tile_dest, tile_src, tile_fill, out_degree, dangling)
        return tuple(pl.pallas_call(
            finish,
            out_shape=(
                jax.ShapeDtypeStruct((share, lanes), jnp.float32),
                jax.ShapeDtypeStruct((ITERS,), jnp.float32),
            ),
            in_specs=[pl.BlockSpec(memory_space=pltpu.VMEM)] * 2,
            out_specs=(pl.BlockSpec(memory_space=pl.ANY),) * 2,
            scratch_shapes=[pltpu.SMEM((ITERS,), jnp.float32), pltpu.SemaphoreType.DMA((2,))],
            compiler_params=pltpu.CompilerParams(vmem_limit_bytes=1 << 20),
        )(rank, changes))

    return jax.shard_map(
        local, mesh=mesh, in_specs=placed, out_specs=(P(("blk", "row"), None), P()), check_vma=False
    )
```

```python
import functools

import jax
import jax.numpy as jnp
from jax import lax
from jax.experimental import pallas as pl
from jax.experimental.pallas import tpu as pltpu
from jax.sharding import PartitionSpec as P

ITERS = 2
UNROLL_LIMIT = 32

damping = 0.85


def each(count, body):
    if count <= UNROLL_LIMIT:
        for i in range(count):
            body(i)
    else:

        @pl.loop(0, count)
        def _(i):
            body(i)


def finish(rank_ref, change_ref, rank_hbm, change_hbm, change_s, sems):
    write_rank = pltpu.make_async_copy(rank_ref, rank_hbm, sems.at[0])
    write_rank.start()
    for i in range(ITERS):
        change_s[i] = jnp.max(change_ref[i:i + 1, :])
    write_change = pltpu.make_async_copy(change_s, change_hbm, sems.at[1])
    write_change.start()
    write_rank.wait()
    write_change.wait()


def kernel(
    n_blk, n_row,
    rank_hbm, tiles_hbm, dest_hbm, src_hbm, fill_hbm, degree_hbm, dangling_hbm,
    rank_out, change_out,
    rank_v, tiles_v, turned_v, degree_v, dangling_v, dest_s, src_s, fill_s,
    weight_v, dangle_v, spread_v, picked_v,
    pages, blk_stats, partial, shares, row_stats, last_stats, in_sems, blk_sems, row_sems, last_sems,
):
    b = lax.axis_index("blk")
    w = lax.axis_index("row")
    share, lanes = rank_v.shape
    slots = tiles_v.shape[0]
    page_total = n_blk * n_row * share * lanes

    def peer(axis, d):
        if axis == "blk":
            return {"blk": lax.rem(b + d, n_blk)}
        if axis == "row":
            return {"row": lax.rem(w + d, n_row)}
        return {"blk": lax.rem(b + d // n_row, n_blk), "row": lax.rem(w + d % n_row, n_row)}

    barrier = pltpu.get_barrier_semaphore()
    for axis, count in (("blk", n_blk), ("row", n_row)):
        each(count - 1, lambda i, axis=axis: pl.semaphore_signal(
            barrier, inc=1, device_id=peer(axis, i + 1),
            device_id_type=pl.DeviceIdType.MESH))

    loads = [
        pltpu.make_async_copy(source, target, in_sems.at[i])
        for i, (source, target) in enumerate((
            (rank_hbm, rank_v), (degree_hbm, degree_v), (dangling_hbm, dangling_v),
            (src_hbm, src_s), (dest_hbm, dest_s), (fill_hbm, fill_s), (tiles_hbm, tiles_v),
        ))
    ]
    for load in loads:
        load.start()
    for load in loads[:3]:
        load.wait()

    def send(axis, count, source, target, sems):
        def one(i):
            d = i + 1
            pltpu.make_async_remote_copy(
                src_ref=source(d), dst_ref=target.at[d],
                send_sem=sems.at[0], recv_sem=sems.at[1],
                device_id=peer(axis, d), device_id_type=pl.DeviceIdType.MESH,
            ).start()

        each(count - 1, one)

    def wait(count, target, sems, which):
        others = target.at[pl.ds(1, count - 1)]
        pltpu.make_async_copy(others, others, sems.at[which]).wait()

    sent = []

    def blk_send(source, target, sems):
        send("blk", n_blk, source, target, sems)
        sent.append((n_blk, target, sems))

    def row_send(source, target, sems):
        send("row", n_row, source, target, sems)
        sent.append((n_row, target, sems))

    def lane_sum(value):
        return jnp.sum(value, axis=0, keepdims=True)

    dangle = dangling_v[...].astype(jnp.float32)
    weight = (1.0 - dangle) / degree_v[...].astype(jnp.float32)
    weight_v[...] = weight
    dangle_v[...] = dangle
    rank = rank_v[...]
    pages[0, 0] = (rank * weight).astype(jnp.bfloat16)
    blk_stats[0, 0] = jnp.concatenate([lane_sum(rank * dangle), jnp.zeros((1, lanes), jnp.float32)], axis=0)
    pl.semaphore_wait(barrier, n_blk + n_row - 2)

    select = None
    for it in range(ITERS):
        blk_send(lambda d: pages.at[it, 0], pages.at[it], blk_sems.at[it, 0])
        blk_send(lambda d: blk_stats.at[it, 0], blk_stats.at[it], blk_sems.at[it, 1])

        if it == 0:
            for load in loads[3:6]:
                load.wait()
            slot_row = lax.broadcasted_iota(jnp.int32, (slots, n_blk * share), 0)
            slot_col = lax.broadcasted_iota(jnp.int32, (slots, n_blk * share), 1)
            source_row = jnp.zeros((slots, n_blk * share), jnp.int32)
            dest_row = lax.broadcasted_iota(jnp.int32, (n_row * share, lanes), 0)
            lane = lax.broadcasted_iota(jnp.int32, (n_row * share, lanes), 1)
            for k in range(slots):
                source = src_s[k]
                place = lax.rem(b - lax.div(source, share) + n_blk, n_blk) * share + lax.rem(source, share)
                source_row = jnp.where(slot_row == k, place, source_row)
                keep = (dest_row == dest_s[k]) & (lane < fill_s[k])
                spread_v[k] = jnp.where(keep, 1.0, 0.0)
            select = jnp.where(source_row == slot_col, 1.0, 0.0).astype(jnp.bfloat16)
            loads[6].wait()
            for k in range(slots):
                turned_v[k] = tiles_v[k].T

        wait(n_blk, pages.at[it], blk_sems.at[it, 0], 1)
        picked_v[...] = jnp.dot(
            select, pages[it].reshape(n_blk * share, lanes), preferred_element_type=jnp.float32
        )
        wait(n_blk, blk_stats.at[it], blk_sems.at[it, 1], 1)
        row_stats[it, 0] = jnp.sum(blk_stats[it], axis=0)
        row_send(lambda d: row_stats.at[it, 0], row_stats.at[it], row_sems.at[it, 1])
        totals = [jnp.zeros((n_row * share, lanes), jnp.float32) for _ in range(2)]
        for k in range(0, slots, 2):
            left = jnp.concatenate([spread_v[k + i] * picked_v[k + i:k + i + 1, :] for i in range(2)], axis=1)
            right = jnp.concatenate([turned_v[k + i] for i in range(2)], axis=0)
            half = k // 2 % 2
            totals[half] = totals[half] + lax.dot_general(
                left.astype(jnp.bfloat16), right, (((1,), (0,)), ((), ())), preferred_element_type=jnp.float32
            )
        partial[it] = (totals[0] + totals[1]).reshape(n_row, share, lanes)
        row_send(lambda d: partial.at[it, lax.rem(w + d, n_row)], shares.at[it], row_sems.at[it, 0])
        own = partial[it, w]
        wait(n_row, row_stats.at[it], row_sems.at[it, 1], 1)
        stats = jnp.sum(jnp.sum(row_stats[it], axis=0), axis=1, keepdims=True)
        if it > 0:
            change_out[0:1, :] = jnp.broadcast_to(stats[1:2, :], (1, lanes))
        base = (1.0 - damping) + damping * stats[0:1, :] / page_total
        wait(n_row, shares.at[it], row_sems.at[it, 0], 1)
        incoming = own + jnp.sum(shares[it, 1:], axis=0)
        updated = damping * incoming + base
        rank = rank_v[...]
        if it == 0:
            rank_v[...] = updated
            pages[it + 1, 0] = (updated * weight_v[...]).astype(jnp.bfloat16)
            blk_stats[it + 1, 0] = jnp.concatenate(
                [lane_sum(updated * dangle_v[...]), lane_sum(jnp.abs(updated - rank))], axis=0
            )
        else:
            last_stats[0] = lane_sum(jnp.abs(updated - rank))
            rank_out[...] = updated

    send("all", n_blk * n_row, lambda d: last_stats.at[0], last_stats, last_sems)
    sent.append((n_blk * n_row, last_stats, last_sems))
    wait(n_blk * n_row, last_stats, last_sems, 1)
    last = jnp.sum(jnp.sum(last_stats[...], axis=0), axis=1, keepdims=True)
    change_out[1:2, :] = jnp.broadcast_to(last, (1, lanes))
    for count, target, sems in sent:
        wait(count, target, sems, 0)


def solution(mesh):
    placed = (
        P(("blk", "row"), None),
        P(("blk", "row"), None, None),
        P(("blk", "row")),
        P(("blk", "row")),
        P(("blk", "row")),
        P(("blk", "row"), None),
        P(("blk", "row"), None),
    )
    n_blk, n_row = mesh.shape["blk"], mesh.shape["row"]

    def local(rank_start, tiles, tile_dest, tile_src, tile_fill, out_degree, dangling):
        share, lanes = rank_start.shape
        slots = tiles.shape[0]
        rank, changes = pl.pallas_call(
            functools.partial(kernel, n_blk, n_row),
            out_shape=(
                pltpu.VMEM((share, lanes), jnp.float32),
                pltpu.VMEM((ITERS, lanes), jnp.float32),
            ),
            in_specs=[pl.BlockSpec(memory_space=pl.ANY)] * 7,
            out_specs=(pl.BlockSpec(memory_space=pltpu.VMEM),) * 2,
            scratch_shapes=[
                pltpu.VMEM((share, lanes), jnp.float32),
                pltpu.VMEM(tiles.shape, jnp.bfloat16),
                pltpu.VMEM(tiles.shape, jnp.bfloat16),
                pltpu.VMEM((share, lanes), jnp.int32),
                pltpu.VMEM((share, lanes), jnp.int32),
                pltpu.SMEM((slots,), jnp.int32),
                pltpu.SMEM((slots,), jnp.int32),
                pltpu.SMEM((slots,), jnp.int32),
                pltpu.VMEM((share, lanes), jnp.float32),
                pltpu.VMEM((share, lanes), jnp.float32),
                pltpu.VMEM((slots, n_row * share, lanes), jnp.float32),
                pltpu.VMEM((slots, lanes), jnp.float32),
                pltpu.VMEM((ITERS, n_blk, share, lanes), jnp.bfloat16),
                pltpu.VMEM((ITERS, n_blk, 2, lanes), jnp.float32),
                pltpu.VMEM((ITERS, n_row, share, lanes), jnp.float32),
                pltpu.VMEM((ITERS, n_row, share, lanes), jnp.float32),
                pltpu.VMEM((ITERS, n_row, 2, lanes), jnp.float32),
                pltpu.VMEM((n_blk * n_row, 1, lanes), jnp.float32),
                pltpu.SemaphoreType.DMA((7,)),
                pltpu.SemaphoreType.DMA((ITERS, 2, 2)),
                pltpu.SemaphoreType.DMA((ITERS, 2, 2)),
                pltpu.SemaphoreType.DMA((2,)),
            ],
            compiler_params=pltpu.CompilerParams(collective_id=0, has_side_effects=True),
        )(rank_start, tiles, tile_dest, tile_src, tile_fill, out_degree, dangling)
        return tuple(pl.pallas_call(
            finish,
            out_shape=(
                jax.ShapeDtypeStruct((share, lanes), jnp.float32),
                jax.ShapeDtypeStruct((ITERS,), jnp.float32),
            ),
            in_specs=[pl.BlockSpec(memory_space=pltpu.VMEM)] * 2,
            out_specs=(pl.BlockSpec(memory_space=pl.ANY),) * 2,
            scratch_shapes=[pltpu.SMEM((ITERS,), jnp.float32), pltpu.SemaphoreType.DMA((2,))],
            compiler_params=pltpu.CompilerParams(vmem_limit_bytes=1 << 20),
        )(rank, changes))

    return jax.shard_map(
        local, mesh=mesh, in_specs=placed, out_specs=(P(("blk", "row"), None), P()), check_vma=False
    )
```

```python
import functools

import jax
import jax.numpy as jnp
from jax import lax
from jax.experimental import pallas as pl
from jax.experimental.pallas import tpu as pltpu
from jax.sharding import PartitionSpec as P

ITERS = 2
UNROLL_LIMIT = 32

damping = 0.85


def each(count, body):
    if count <= UNROLL_LIMIT:
        for i in range(count):
            body(i)
    else:

        @pl.loop(0, count)
        def _(i):
            body(i)


def finish(rank_ref, change_ref, rank_hbm, change_hbm, sems):
    writes = [
        pltpu.make_async_copy(source, target, sems.at[i])
        for i, (source, target) in enumerate(((rank_ref, rank_hbm), (change_ref, change_hbm)))
    ]
    for write in writes:
        write.start()
    for write in writes:
        write.wait()


def kernel(
    n_blk, n_row,
    rank_hbm, tiles_hbm, dest_hbm, src_hbm, fill_hbm, degree_hbm, dangling_hbm,
    rank_out, change_out,
    rank_v, tiles_v, turned_v, degree_v, dangling_v, dest_s, src_s, fill_s,
    weight_v, dangle_v, spread_v, picked_v,
    pages, blk_stats, partial, shares, row_stats, last_stats, in_sems, blk_sems, row_sems, last_sems,
):
    b = lax.axis_index("blk")
    w = lax.axis_index("row")
    share, lanes = rank_v.shape
    slots = tiles_v.shape[0]
    page_total = n_blk * n_row * share * lanes

    def peer(axis, d):
        if axis == "blk":
            return {"blk": lax.rem(b + d, n_blk)}
        if axis == "row":
            return {"row": lax.rem(w + d, n_row)}
        return {"blk": lax.rem(b + d // n_row, n_blk), "row": lax.rem(w + d % n_row, n_row)}

    barrier = pltpu.get_barrier_semaphore()
    for axis, count in (("blk", n_blk), ("row", n_row)):
        each(count - 1, lambda i, axis=axis: pl.semaphore_signal(
            barrier, inc=1, device_id=peer(axis, i + 1),
            device_id_type=pl.DeviceIdType.MESH))

    loads = [
        pltpu.make_async_copy(source, target, in_sems.at[i])
        for i, (source, target) in enumerate((
            (rank_hbm, rank_v), (degree_hbm, degree_v), (dangling_hbm, dangling_v),
            (src_hbm, src_s), (dest_hbm, dest_s), (fill_hbm, fill_s), (tiles_hbm, tiles_v),
        ))
    ]
    for load in loads:
        load.start()
    for load in loads[:3]:
        load.wait()

    def send(axis, count, source, target, sems):
        def one(i):
            d = i + 1
            pltpu.make_async_remote_copy(
                src_ref=source(d), dst_ref=target.at[d],
                send_sem=sems.at[0], recv_sem=sems.at[1],
                device_id=peer(axis, d), device_id_type=pl.DeviceIdType.MESH,
            ).start()

        each(count - 1, one)

    def wait(count, target, sems, which):
        others = target.at[pl.ds(1, count - 1)]
        pltpu.make_async_copy(others, others, sems.at[which]).wait()

    sent = []

    def blk_send(source, target, sems):
        send("blk", n_blk, source, target, sems)
        sent.append((n_blk, target, sems))

    def row_send(source, target, sems):
        send("row", n_row, source, target, sems)
        sent.append((n_row, target, sems))

    def lane_sum(value):
        return jnp.sum(value, axis=0, keepdims=True)

    dangle = dangling_v[...].astype(jnp.float32)
    weight = (1.0 - dangle) / degree_v[...].astype(jnp.float32)
    weight_v[...] = weight
    dangle_v[...] = dangle
    rank = rank_v[...]
    pages[0, 0] = (rank * weight).astype(jnp.bfloat16)
    blk_stats[0, 0] = jnp.concatenate([lane_sum(rank * dangle), jnp.zeros((1, lanes), jnp.float32)], axis=0)
    pl.semaphore_wait(barrier, n_blk + n_row - 2)

    select = None
    order = lax.broadcasted_iota(jnp.int32, (1, ITERS), 1)
    moves = jnp.zeros((1, ITERS), jnp.float32)
    for it in range(ITERS):
        blk_send(lambda d: pages.at[it, 0], pages.at[it], blk_sems.at[it, 0])
        blk_send(lambda d: blk_stats.at[it, 0], blk_stats.at[it], blk_sems.at[it, 1])

        if it == 0:
            for load in loads[3:6]:
                load.wait()
            slot_row = lax.broadcasted_iota(jnp.int32, (slots, n_blk * share), 0)
            slot_col = lax.broadcasted_iota(jnp.int32, (slots, n_blk * share), 1)
            source_row = jnp.zeros((slots, n_blk * share), jnp.int32)
            dest_row = lax.broadcasted_iota(jnp.int32, (n_row * share, lanes), 0)
            lane = lax.broadcasted_iota(jnp.int32, (n_row * share, lanes), 1)
            for k in range(slots):
                source = src_s[k]
                place = lax.rem(b - lax.div(source, share) + n_blk, n_blk) * share + lax.rem(source, share)
                source_row = jnp.where(slot_row == k, place, source_row)
                keep = (dest_row == dest_s[k]) & (lane < fill_s[k])
                spread_v[k] = jnp.where(keep, 1.0, 0.0)
            select = jnp.where(source_row == slot_col, 1.0, 0.0).astype(jnp.bfloat16)
            loads[6].wait()
            for k in range(slots):
                turned_v[k] = tiles_v[k].T

        wait(n_blk, pages.at[it], blk_sems.at[it, 0], 1)
        picked_v[...] = jnp.dot(
            select, pages[it].reshape(n_blk * share, lanes), preferred_element_type=jnp.float32
        )
        wait(n_blk, blk_stats.at[it], blk_sems.at[it, 1], 1)
        row_stats[it, 0] = jnp.sum(blk_stats[it], axis=0)
        row_send(lambda d: row_stats.at[it, 0], row_stats.at[it], row_sems.at[it, 1])
        totals = [jnp.zeros((n_row * share, lanes), jnp.float32) for _ in range(2)]
        for k in range(0, slots, 2):
            left = jnp.concatenate([spread_v[k + i] * picked_v[k + i:k + i + 1, :] for i in range(2)], axis=1)
            right = jnp.concatenate([turned_v[k + i] for i in range(2)], axis=0)
            half = k // 2 % 2
            totals[half] = totals[half] + lax.dot_general(
                left.astype(jnp.bfloat16), right, (((1,), (0,)), ((), ())), preferred_element_type=jnp.float32
            )
        partial[it] = (totals[0] + totals[1]).reshape(n_row, share, lanes)
        row_send(lambda d: partial.at[it, lax.rem(w + d, n_row)], shares.at[it], row_sems.at[it, 0])
        own = partial[it, w]
        wait(n_row, row_stats.at[it], row_sems.at[it, 1], 1)
        stats = jnp.sum(jnp.sum(row_stats[it], axis=0), axis=1, keepdims=True)
        if it > 0:
            moves = jnp.where(order == it - 1, stats[1:2, :], moves)
        base = (1.0 - damping) + damping * stats[0:1, :] / page_total
        wait(n_row, shares.at[it], row_sems.at[it, 0], 1)
        incoming = own + jnp.sum(shares[it, 1:], axis=0)
        updated = damping * incoming + base
        rank = rank_v[...]
        if it == 0:
            rank_v[...] = updated
            pages[it + 1, 0] = (updated * weight_v[...]).astype(jnp.bfloat16)
            blk_stats[it + 1, 0] = jnp.concatenate(
                [lane_sum(updated * dangle_v[...]), lane_sum(jnp.abs(updated - rank))], axis=0
            )
        else:
            last_stats[0] = lane_sum(jnp.abs(updated - rank))
            rank_out[...] = updated

    send("all", n_blk * n_row, lambda d: last_stats.at[0], last_stats, last_sems)
    sent.append((n_blk * n_row, last_stats, last_sems))
    wait(n_blk * n_row, last_stats, last_sems, 1)
    last = jnp.sum(jnp.sum(last_stats[...], axis=0), axis=1, keepdims=True)
    change_out[...] = jnp.where(order == ITERS - 1, last, moves)
    for count, target, sems in sent:
        wait(count, target, sems, 0)


def solution(mesh):
    placed = (
        P(("blk", "row"), None),
        P(("blk", "row"), None, None),
        P(("blk", "row")),
        P(("blk", "row")),
        P(("blk", "row")),
        P(("blk", "row"), None),
        P(("blk", "row"), None),
    )
    n_blk, n_row = mesh.shape["blk"], mesh.shape["row"]

    def local(rank_start, tiles, tile_dest, tile_src, tile_fill, out_degree, dangling):
        share, lanes = rank_start.shape
        slots = tiles.shape[0]
        rank, changes = pl.pallas_call(
            functools.partial(kernel, n_blk, n_row),
            out_shape=(
                pltpu.VMEM((share, lanes), jnp.float32),
                pltpu.VMEM((1, ITERS), jnp.float32),
            ),
            in_specs=[pl.BlockSpec(memory_space=pl.ANY)] * 7,
            out_specs=(pl.BlockSpec(memory_space=pltpu.VMEM),) * 2,
            scratch_shapes=[
                pltpu.VMEM((share, lanes), jnp.float32),
                pltpu.VMEM(tiles.shape, jnp.bfloat16),
                pltpu.VMEM(tiles.shape, jnp.bfloat16),
                pltpu.VMEM((share, lanes), jnp.int32),
                pltpu.VMEM((share, lanes), jnp.int32),
                pltpu.SMEM((slots,), jnp.int32),
                pltpu.SMEM((slots,), jnp.int32),
                pltpu.SMEM((slots,), jnp.int32),
                pltpu.VMEM((share, lanes), jnp.float32),
                pltpu.VMEM((share, lanes), jnp.float32),
                pltpu.VMEM((slots, n_row * share, lanes), jnp.float32),
                pltpu.VMEM((slots, lanes), jnp.float32),
                pltpu.VMEM((ITERS, n_blk, share, lanes), jnp.bfloat16),
                pltpu.VMEM((ITERS, n_blk, 2, lanes), jnp.float32),
                pltpu.VMEM((ITERS, n_row, share, lanes), jnp.float32),
                pltpu.VMEM((ITERS, n_row, share, lanes), jnp.float32),
                pltpu.VMEM((ITERS, n_row, 2, lanes), jnp.float32),
                pltpu.VMEM((n_blk * n_row, 1, lanes), jnp.float32),
                pltpu.SemaphoreType.DMA((7,)),
                pltpu.SemaphoreType.DMA((ITERS, 2, 2)),
                pltpu.SemaphoreType.DMA((ITERS, 2, 2)),
                pltpu.SemaphoreType.DMA((2,)),
            ],
            compiler_params=pltpu.CompilerParams(collective_id=0, has_side_effects=True),
        )(rank_start, tiles, tile_dest, tile_src, tile_fill, out_degree, dangling)
        rank, changes = pl.pallas_call(
            finish,
            out_shape=(
                jax.ShapeDtypeStruct((share, lanes), jnp.float32),
                jax.ShapeDtypeStruct((1, ITERS), jnp.float32),
            ),
            in_specs=[pl.BlockSpec(memory_space=pltpu.VMEM)] * 2,
            out_specs=(pl.BlockSpec(memory_space=pl.ANY),) * 2,
            scratch_shapes=[pltpu.SemaphoreType.DMA((2,))],
            compiler_params=pltpu.CompilerParams(vmem_limit_bytes=1 << 20),
        )(rank, changes)
        return rank, changes.reshape(ITERS)

    return jax.shard_map(
        local, mesh=mesh, in_specs=placed, out_specs=(P(("blk", "row"), None), P()), check_vma=False
    )
```
